256 devices in a mesh: grp: 8 (over y, core), blk: 32 (over x, z).
Axes of the slice: x: 4, y: 4, z: 8, core: 2. Of those that a mesh axis runs over, the one named last changes fastest.
Arguments:
- node_vars: bfloat16 [112, 98304], P(None, ('grp', 'blk')), may hold values from -6 to 6
- w_in: bfloat16 [512, 112], replicated, may hold values from -0.5 to 0.5
- w_out: bfloat16 [96, 512], replicated, may hold values from -0.25 to 0.25
- linear_part: bfloat16 [96, 112], replicated, may hold values from -0.1875 to 0.1875
- step_len: float32 [512, 8], P(('grp', 'blk')), may hold values from 0.02 to 1.08
- path_count: int32 [512, 8], P(('grp', 'blk')), may hold values from 1 to 16, as said below
- path_node: int32 [512, 8, 16], P(('grp', 'blk')), may hold values from 0 to 23
- path_con: int32 [512, 8, 16], P(('grp', 'blk')), may hold values from 0 to 95
Outputs:
- tangent: bfloat16 [98304, 10752], P(('grp', 'blk'))
- path_rows: bfloat16 [112, 65536], P(None, ('grp', 'blk'))
- row_start: int32 [256], P(('grp', 'blk'))
The draws below stay inside these ranges and needn't reach their ends.
Inputs may be any that keep to these rules, and one draw needn't show every extreme that they name: `path_count`: the path-constraint rows of one device number at most 256, and in every group one device has exactly that many.
All inputs are finite; a program needn't handle non-finite values.
Results may differ from the reference program's by a relative error of at most 0.0012.
The reference program's roundings to bfloat16 on the way (of `scaled` and `path_entry`) count: a program that leaves them out, or rounds other values in their place, can miss the bound.
Values may be sent and summed in bfloat16 or wider, within the bound.
A program may use at most 192 MiB of HBM per device.

```python
import jax
import jax.numpy as jnp
from jax import lax

STATES = 96
UNITS = 512
NODES = 24
MAXP = 16
TRAJ = 8
INT_DEV = 2
VARS = 112
INTERVALS = 512
NODE_ROWS = 98304
PATH_ROWS = 65536
GROUP_SLOTS = 8192
N_GRP = 8
N_BLK = 32


def draw_node_vars(key, part):
    subkeys = jax.random.split(key, 4)
    pair_total = INTERVALS * TRAJ
    group_total = INTERVALS // (INT_DEV * N_BLK)
    span = jnp.log(75.0) / 3.0
    group_level = jax.random.uniform(subkeys[0], (group_total,), jnp.float32, 0.0, 1.0) * span
    pair_level = jax.random.uniform(subkeys[1], (pair_total,), jnp.float32, 0.0, 1.0) * span
    node_level = jax.random.uniform(subkeys[2], (NODE_ROWS,), jnp.float32, 0.0, 1.0) * span
    group_of_pair = jnp.arange(pair_total, dtype=jnp.int32) // (N_BLK * INT_DEV * TRAJ)
    level = jnp.repeat(group_level[group_of_pair] + pair_level, NODES) + node_level
    spread = 0.08 * jnp.exp(level)
    base = 0.55 * jax.random.truncated_normal(subkeys[3], -1.8, 1.8, (VARS, NODE_ROWS), jnp.float32)
    return (base * spread[None, :]).astype(jnp.bfloat16)


def draw_step_len(key, part):
    subkeys = jax.random.split(key, 2)
    devices = INTERVALS // INT_DEV
    position = jnp.arange(INTERVALS, dtype=jnp.float32)[:, None] / INTERVALS
    heavy = jax.random.randint(subkeys[1], (devices,), 0, INT_DEV * TRAJ)
    is_heavy = (jnp.arange(INT_DEV * TRAJ, dtype=jnp.int32)[None, :] == heavy[:, None]).reshape(INTERVALS, TRAJ)
    roughness = jax.random.uniform(subkeys[0], (INTERVALS, TRAJ), jnp.float32, 1.0, 3.0)
    growth = 3.0 ** position
    boost = jnp.where(is_heavy, 6.0, 1.0)
    return (0.02 * growth * roughness * boost).astype(jnp.float32)


def draw_path_count(key, part):
    subkeys = jax.random.split(key, 3)
    devices = INTERVALS // INT_DEV
    ceiling = jax.random.randint(subkeys[0], (devices,), max(MAXP // 4, 1), MAXP + 1)
    busiest = jax.random.randint(subkeys[1], (devices // N_BLK,), 0, N_BLK)
    is_busy = jnp.arange(devices) % N_BLK == jnp.repeat(busiest, N_BLK)
    ceiling = jnp.where(is_busy, MAXP, ceiling)
    per_row = jnp.repeat(ceiling, INT_DEV)[:, None]
    counts = jax.random.randint(subkeys[2], (INTERVALS, TRAJ), 1, per_row + 1)
    counts = jnp.where(jnp.repeat(is_busy, INT_DEV)[:, None], MAXP, counts)
    return counts.astype(jnp.int32)


def plant(result, key, low, top_value):
    longest = result.shape.index(max(result.shape))
    spots = []
    for shift in (0, 1):
        where = [jax.random.randint(jax.random.fold_in(key, axis), (), 0, length) for axis, length in enumerate(result.shape)]
        where[longest] = (where[longest] + shift) % result.shape[longest]
        spots.append(tuple(where))
    return result.at[spots[0]].set(low).at[spots[1]].set(top_value)


def gaussian(stream_key, extent, scale, bound, kind=jnp.bfloat16):
    values = scale * jax.random.normal(stream_key, extent, jnp.float32)
    return jnp.clip(values, min=-bound, max=bound).astype(kind)


def setup_inputs(seed: int = 0) -> dict:
    key_of = jax.random.split(jax.random.key(seed), 9)
    return {
        "node_vars": draw_node_vars(jax.random.fold_in(key_of[8], 71), 0),
        "w_in": gaussian(key_of[1], (UNITS, VARS), VARS ** -0.5, 0.5),
        "w_out": gaussian(key_of[2], (STATES, UNITS), UNITS ** -0.5, 0.25),
        "linear_part": gaussian(key_of[3], (STATES, VARS), (8 * VARS) ** -0.5, 0.1875),
        "step_len": draw_step_len(jax.random.fold_in(key_of[8], 71), 0),
        "path_count": draw_path_count(jax.random.fold_in(key_of[8], 71), 0),
        "path_node": plant(jax.random.randint(key_of[6], (INTERVALS, TRAJ, MAXP), 0, NODES), jax.random.fold_in(key_of[6], 1), 0, NODES - 1).astype(jnp.int32),
        "path_con": plant(jax.random.randint(key_of[7], (INTERVALS, TRAJ, MAXP), 0, STATES), jax.random.fold_in(key_of[7], 1), 0, STATES - 1).astype(jnp.int32),
    }


def node_blocks(vars_block, w_in, w_out, linear_part):
    preact = jnp.dot(w_in, vars_block, preferred_element_type=jnp.float32)
    slopes = 1.0 - jnp.tanh(preact) ** 2
    scaled = (w_out.astype(jnp.float32)[None, :, :] * slopes.T[:, None, :]).astype(jnp.bfloat16)
    node_count = scaled.shape[0]
    products = jnp.dot(scaled.reshape(node_count * STATES, UNITS), w_in, preferred_element_type=jnp.float32)
    return products.reshape(node_count, STATES, VARS) + linear_part.astype(jnp.float32)[None, :, :]

def reference(node_vars, w_in, w_out, linear_part, step_len, path_count, path_node, path_con):
    block_rows = INT_DEV * TRAJ * NODES
    block_total = NODE_ROWS // block_rows
    vars_blocks = node_vars.reshape(VARS, block_total, block_rows).transpose(1, 0, 2)
    half_step = jnp.repeat(step_len.reshape(-1) * 0.5, NODES).reshape(block_total, block_rows)

    def add_squares(running, inputs):
        vars_block, half_block = inputs
        defect = half_block[:, None, None] * node_blocks(vars_block, w_in, w_out, linear_part)
        return (running + lax.optimization_barrier(jnp.sum(defect * defect, axis=(0, 1))), None)
    column_sq, unused = lax.scan(add_squares, jnp.zeros((VARS,), jnp.float32), (vars_blocks, half_step))
    column_norm = jnp.sqrt(column_sq / (NODE_ROWS * STATES) + 1e-06)

    def scaled_block(inputs):
        vars_block, half_block = inputs
        defect = half_block[:, None, None] * node_blocks(vars_block, w_in, w_out, linear_part)
        return (defect / column_norm[None, None, :]).astype(jnp.bfloat16).reshape(block_rows, STATES * VARS)
    tangent = lax.map(scaled_block, (vars_blocks, half_step)).reshape(NODE_ROWS, STATES * VARS)
    pair_total = INTERVALS * TRAJ
    counts = path_count.reshape(pair_total)
    slot_index = jnp.arange(MAXP, dtype=jnp.int32)
    node_index = (jnp.arange(pair_total, dtype=jnp.int32)[:, None] * NODES + path_node.reshape(pair_total, MAXP)).reshape(-1)
    con_index = path_con.reshape(-1)
    preact = jnp.dot(w_in, node_vars, preferred_element_type=jnp.float32)
    picked = (1.0 - jnp.tanh(preact[:, node_index]) ** 2).T
    scaled_rows = (w_out.astype(jnp.float32)[con_index] * picked).astype(jnp.bfloat16)
    path_entry = (jnp.dot(scaled_rows, w_in, preferred_element_type=jnp.float32) + linear_part.astype(jnp.float32)[con_index]).astype(jnp.bfloat16)
    earlier = (jnp.cumsum(counts) - counts).astype(jnp.int32)
    group_pairs = N_BLK * INT_DEV * TRAJ
    group_first = earlier.reshape(N_GRP, group_pairs)[:, 0]
    group_id = (jnp.arange(pair_total, dtype=jnp.int32) // group_pairs).astype(jnp.int32)
    position = (earlier - group_first[group_id]).astype(jnp.int32)
    numbered = (position[:, None] + slot_index[None, :]).astype(jnp.int32)
    column = group_id[:, None] * GROUP_SLOTS + numbered % N_BLK * (GROUP_SLOTS // N_BLK) + numbered // N_BLK
    column = jnp.where(slot_index[None, :] < counts[:, None], column, PATH_ROWS).astype(jnp.int32).reshape(-1)
    path_rows = jnp.zeros((PATH_ROWS, VARS), jnp.bfloat16).at[column].set(path_entry, mode='drop').T
    device_total = lax.optimization_barrier(jnp.sum(counts.reshape(INTERVALS // INT_DEV, INT_DEV * TRAJ), axis=1)).astype(jnp.int32)
    row_start = (jnp.cumsum(device_total) - device_total).astype(jnp.int32)
    return (tangent, path_rows, row_start)
```

```python
import functools

import jax
import jax.numpy as jnp
from jax import lax
from jax.experimental import pallas as pl
from jax.experimental.pallas import tpu as pltpu
from jax.sharding import PartitionSpec as P

STATES = 96
UNITS = 512
NODES = 24
MAXP = 16
VARS = 112
LANES = 128
GROUP = 8
STEPS = STATES // GROUP
SENT_ROWS = 8
EARLY = 2
MESH = pl.DeviceIdType.MESH
BF16 = jnp.bfloat16
F32 = jnp.float32


def dot(a, b, dims):
    return lax.dot_general(a, b, (dims, ((), ())), preferred_element_type=F32)


def nn(a, b):
    return dot(a, b, ((1,), (0,)))


def nt(a, b):
    return dot(a, b, ((1,), (1,)))


def tn(a, b):
    return dot(a, b, ((0,), (0,)))


def iota(shape, axis):
    return lax.broadcasted_iota(jnp.int32, shape, axis)


def split2(x):
    high = x.astype(BF16)
    return high, (x - high.astype(F32)).astype(BF16)


def split3(x):
    high = x.astype(BF16)
    rest = x - high.astype(F32)
    mid = rest.astype(BF16)
    return high, mid, (rest - mid.astype(F32)).astype(BF16)


def front(
    n_grp, n_blk,
    vars_ref, w_in_t_ref, w_out_ref, linear_ref, step_ref, count_ref, node_ref, con_ref,
    defect_ref, inv_ref, place_ref, rows_ref, start_ref,
    slopes, w_cols, l_cols, half_row, entry, msg1, recv1, msg2, recv2, send_rows, recv_rows,
    s1_send, s1_recv, s2_send, s2_recv, s3_send, s3_recv,
):
    grp, blk = lax.axis_index("grp"), lax.axis_index("blk")
    pairs = count_ref.shape[0] * count_ref.shape[1]
    traj = count_ref.shape[1]
    rows = vars_ref.shape[1]
    slots = pairs * MAXP

    barrier = pltpu.get_barrier_semaphore()

    @pl.loop(1, n_blk)
    def _(i):
        pl.semaphore_signal(barrier, inc=1, device_id={"blk": lax.rem(blk + i, n_blk)}, device_id_type=MESH)

    @pl.loop(1, n_grp)
    def _(i):
        pl.semaphore_signal(barrier, inc=1, device_id={"grp": lax.rem(grp + i, n_grp)}, device_id_type=MESH)

    w_in_t = w_in_t_ref[...]
    w_out = w_out_ref[...]
    linear = linear_ref[...]
    preact = tn(w_in_t, vars_ref[...])
    th = jnp.tanh(preact)
    slopes[...] = 1.0 - th * th

    row_pair = iota((1, rows), 1) // NODES
    half = jnp.zeros((1, rows), F32)
    for e in range(pairs):
        half = jnp.where(row_pair == e, step_ref[e // traj, e % traj] * 0.5, half)
    half_row[...] = half

    scaled = slopes[...] * half
    high, low = split2(scaled)
    gram = nt(high, high) + 2.0 * nt(high, low)
    m_high, m_low = split2(tn(w_out, w_out) * gram)
    w_in = w_in_t.astype(F32).T
    w_in16 = w_in.astype(BF16)
    inner = nn(m_high, w_in16) + nn(m_low, w_in16)
    cross = jnp.sum(scaled * half, axis=1, keepdims=True) * tn(w_out, linear)
    linear32 = linear.astype(F32)
    column = jnp.sum(w_in * (inner + 2.0 * cross), axis=0, keepdims=True)
    column += jnp.sum(half * half) * jnp.sum(linear32 * linear32, axis=0, keepdims=True)

    own_total = jnp.int32(0)
    befores = []
    for e in range(pairs):
        befores.append(own_total)
        own_total += count_ref[e // traj, e % traj]
    tail = jnp.where(iota((1, LANES - VARS), 1) == 0, own_total.astype(F32), 0.0)
    message = jnp.concatenate([column, tail], axis=1)
    msg1[0] = message
    recv1[blk] = message

    w_t = w_out.astype(F32).T
    l_t = linear32.T
    for g in range(STEPS):
        w_cols[g] = w_t[:, g * GROUP:(g + 1) * GROUP]
        l_cols[g] = l_t[:, g * GROUP:(g + 1) * GROUP]

    def main(g):
        for k in range(0, GROUP, 2):
            cols = w_cols[g]
            here = slopes[...]
            block = jnp.concatenate([here * cols[:, k:k + 1], here * cols[:, k + 1:k + 2]], axis=1)
            product = nn(w_in_t, block.astype(BF16))
            lin = l_cols[g]
            for j in range(2):
                part = product[:, j * rows:(j + 1) * rows] + lin[:, k + j:k + j + 1]
                defect_ref[g * GROUP + k + j] = part * half_row[...]

    slot_pair = iota((slots, 1), 0) // MAXP
    slot_k = iota((slots, 1), 0) % MAXP
    count = jnp.zeros((slots, 1), jnp.int32)
    before = jnp.zeros((slots, 1), jnp.int32)
    for e in range(pairs):
        count = jnp.where(slot_pair == e, count_ref[e // traj, e % traj], count)
        before = jnp.where(slot_pair == e, befores[e], before)
    number = jnp.where(slot_k < count, before + slot_k, -1)

    def by_slot(ref):
        table = ref[...].reshape(pairs, 1, MAXP).astype(F32)
        wide = jnp.broadcast_to(table, (pairs, MAXP, MAXP)).reshape(slots, MAXP)
        mine = iota((slots, MAXP), 1) == slot_k
        return jnp.sum(jnp.where(mine, wide, 0.0), axis=1, keepdims=True).astype(jnp.int32)

    node = slot_pair * NODES + by_slot(node_ref)
    con = by_slot(con_ref)
    pick_node = (iota((slots, rows), 1) == node).astype(F32).astype(BF16)
    pick_con = (iota((slots, STATES), 1) == con).astype(F32).astype(BF16)
    s_high, s_mid, s_low = split3(slopes[...])
    slope_rows = nt(pick_node, s_high) + (nt(pick_node, s_mid) + nt(pick_node, s_low))
    scaled_rows = (nn(pick_con, w_out) * slope_rows).astype(BF16)
    entry_rows = nt(scaled_rows, w_in_t) + nn(pick_con, linear)
    entry[...] = jnp.concatenate([entry_rows, jnp.zeros((slots, LANES - VARS), F32)], axis=1).astype(BF16)

    @pl.loop(0, EARLY)
    def _(g):
        main(g)

    pl.semaphore_wait(barrier, n_blk + n_grp - 2)

    def copy1(i):
        peer = lax.rem(blk + i, n_blk)
        return pltpu.make_async_remote_copy(
            src_ref=msg1.at[0], dst_ref=recv1.at[blk], send_sem=s1_send.at[peer], recv_sem=s1_recv.at[blk],
            device_id={"blk": peer}, device_id_type=MESH)

    @pl.loop(1, n_blk)
    def _(i):
        copy1(i).start()

    @pl.loop(EARLY, STEPS)
    def _(g):
        main(g)

    @pl.loop(1, n_blk)
    def _(i):
        peer = lax.rem(blk + i, n_blk)
        pltpu.make_async_remote_copy(
            src_ref=msg1.at[0], dst_ref=recv1.at[peer], send_sem=s1_send.at[peer], recv_sem=s1_recv.at[peer],
            device_id={"blk": peer}, device_id_type=MESH).wait_recv()

    table = recv1[...].reshape(n_blk, LANES)
    message2 = jnp.sum(table, axis=0, keepdims=True)
    msg2[0] = message2
    recv2[grp] = message2

    def copy2(i):
        peer = lax.rem(grp + i, n_grp)
        return pltpu.make_async_remote_copy(
            src_ref=msg2.at[0], dst_ref=recv2.at[grp], send_sem=s2_send.at[peer], recv_sem=s2_recv.at[grp],
            device_id={"grp": peer}, device_id_type=MESH)

    @pl.loop(1, n_grp)
    def _(i):
        copy2(i).start()

    earlier = (iota((n_blk, n_blk), 1) < iota((n_blk, n_blk), 0)).astype(F32).astype(BF16)
    total32 = table[:, VARS:VARS + 1]
    firsts = nn(earlier, table.astype(BF16))[:, VARS:VARS + 1].astype(jnp.int32)
    totals = total32.astype(jnp.int32)
    mine = iota((n_blk, 1), 0) == blk
    first = jnp.sum(jnp.where(mine, firsts, 0))

    q = iota((1, n_blk * SENT_ROWS), 1)
    wanted = lax.rem(q // SENT_ROWS + n_blk * MAXP * pairs - first, n_blk) + n_blk * (q % SENT_ROWS)
    move = (number == wanted).astype(F32).astype(BF16)
    moved = tn(move, entry[...]).astype(BF16).reshape(n_blk, SENT_ROWS, LANES)
    send_rows[...] = moved

    def copy3(i):
        peer = lax.rem(blk + i, n_blk)
        return pltpu.make_async_remote_copy(
            src_ref=send_rows.at[peer], dst_ref=recv_rows.at[blk], send_sem=s3_send.at[peer], recv_sem=s3_recv.at[blk],
            device_id={"blk": peer}, device_id_type=MESH)

    @pl.loop(1, n_blk)
    def _(i):
        copy3(i).start()

    recv_rows[blk] = send_rows[blk]

    skip = lax.rem(blk + n_blk * MAXP * pairs - firsts, n_blk)
    slot0 = (firsts + skip) // n_blk
    live_rows = (totals - skip + n_blk - 1) // n_blk

    def by_row(x):
        return jnp.broadcast_to(x.astype(F32).reshape(n_blk, 1, 1), (n_blk, SENT_ROWS, 1)).reshape(n_blk * SENT_ROWS, 1).astype(jnp.int32)

    k_row = iota((n_blk * SENT_ROWS, 1), 0) % SENT_ROWS
    slot_row = jnp.where(k_row < by_row(live_rows), by_row(slot0) + k_row, -1)
    place_ref[...] = (iota((n_blk * SENT_ROWS, slots), 1) == slot_row).astype(F32).astype(BF16)

    @pl.loop(1, n_grp)
    def _(i):
        peer = lax.rem(grp + i, n_grp)
        pltpu.make_async_remote_copy(
            src_ref=msg2.at[0], dst_ref=recv2.at[peer], send_sem=s2_send.at[peer], recv_sem=s2_recv.at[peer],
            device_id={"grp": peer}, device_id_type=MESH).wait_recv()

    table2 = recv2[...].reshape(n_grp, LANES)
    earlier_groups = jnp.where(iota((n_grp, 1), 0) < grp, table2[:, VARS:VARS + 1], 0.0)
    start_ref[0] = jnp.sum(earlier_groups).astype(jnp.int32) + first
    column_sq = jnp.sum(table2, axis=0, keepdims=True)
    entries = rows * n_grp * n_blk * STATES
    inverse = 1.0 / jnp.sqrt(column_sq / entries + 1e-06)
    inv_ref[...] = jnp.broadcast_to(inverse, (LANES, LANES)).T[:VARS]

    @pl.loop(1, n_blk)
    def _(i):
        peer = lax.rem(blk + i, n_blk)
        pltpu.make_async_remote_copy(
            src_ref=send_rows.at[peer], dst_ref=recv_rows.at[peer], send_sem=s3_send.at[peer], recv_sem=s3_recv.at[peer],
            device_id={"blk": peer}, device_id_type=MESH).wait_recv()

    rows_ref[...] = recv_rows[...]

    @pl.loop(1, n_blk)
    def _(i):
        copy1(i).wait_send()
        copy3(i).wait_send()

    @pl.loop(1, n_grp)
    def _(i):
        copy2(i).wait_send()


def back(defect_ref, inv_ref, place_ref, rows_ref, first_ref, tangent_ref, path_ref, start_ref):
    g = pl.program_id(0)

    @pl.when(g == 0)
    def _():
        start_ref[0] = first_ref[0]
        received = rows_ref[...].reshape(rows_ref.shape[0] * rows_ref.shape[1], LANES)
        path_ref[...] = tn(received, place_ref[...])[:VARS].astype(BF16)

    rows = defect_ref.shape[2]
    inv = jnp.concatenate([inv_ref[...]] * (rows // LANES), axis=1)
    block = (defect_ref[pl.ds(g * GROUP, GROUP)] * inv[None]).astype(BF16)
    tangent_ref[...] = block.reshape(GROUP * VARS, rows).T


def local(n_grp, n_blk, node_vars, w_in, w_out, linear_part, step_len, path_count, path_node, path_con):
    rows = node_vars.shape[1]
    slots = path_count.shape[0] * path_count.shape[1] * MAXP
    vmem = pl.BlockSpec(memory_space=pltpu.VMEM)
    smem = pl.BlockSpec(memory_space=pltpu.SMEM)
    dma = pltpu.SemaphoreType.DMA
    defect, inv, place, received, first = pl.pallas_call(
        functools.partial(front, n_grp, n_blk),
        out_shape=(
            pltpu.VMEM((STATES, VARS, rows), F32),
            pltpu.VMEM((VARS, LANES), F32),
            pltpu.VMEM((n_blk * SENT_ROWS, slots), BF16),
            pltpu.VMEM((n_blk, SENT_ROWS, LANES), BF16),
            jax.ShapeDtypeStruct((1,), jnp.int32),
        ),
        in_specs=[vmem, vmem, vmem, vmem, smem, smem, vmem, vmem],
        out_specs=(vmem, vmem, vmem, vmem, smem),
        scratch_shapes=[
            pltpu.VMEM((UNITS, rows), F32),
            pltpu.VMEM((STEPS, UNITS, GROUP), F32),
            pltpu.VMEM((STEPS, VARS, GROUP), F32),
            pltpu.VMEM((1, rows), F32),
            pltpu.VMEM((slots, LANES), BF16),
            pltpu.VMEM((1, 1, LANES), F32),
            pltpu.VMEM((n_blk, 1, LANES), F32),
            pltpu.VMEM((1, 1, LANES), F32),
            pltpu.VMEM((n_grp, 1, LANES), F32),
            pltpu.VMEM((n_blk, SENT_ROWS, LANES), BF16),
            pltpu.VMEM((n_blk, SENT_ROWS, LANES), BF16),
            dma((n_blk,)), dma((n_blk,)), dma((n_grp,)), dma((n_grp,)), dma((n_blk,)), dma((n_blk,)),
        ],
        compiler_params=pltpu.CompilerParams(collective_id=0, has_side_effects=True, vmem_limit_bytes=40 * 2**20),
        name="front",
    )(node_vars, w_in.T, w_out, linear_part, step_len, path_count, path_node, path_con)
    return pl.pallas_call(
        back,
        grid=(STEPS,),
        out_shape=(
            jax.ShapeDtypeStruct((rows, STATES * VARS), BF16),
            jax.ShapeDtypeStruct((VARS, slots), BF16),
            jax.ShapeDtypeStruct((1,), jnp.int32),
        ),
        in_specs=[vmem, vmem, vmem, vmem, smem],
        out_specs=(
            pl.BlockSpec((rows, GROUP * VARS), lambda g: (0, g)),
            pl.BlockSpec((VARS, slots), lambda g: (0, 0)),
            smem,
        ),
        compiler_params=pltpu.CompilerParams(vmem_limit_bytes=16 * 2**20),
        name="back",
    )(defect, inv, place, received, first)


def solution(mesh):
    both = ("grp", "blk")
    return jax.shard_map(
        functools.partial(local, mesh.shape["grp"], mesh.shape["blk"]),
        mesh=mesh,
        in_specs=(
            P(None, both),
            P(),
            P(),
            P(),
            P(both, None),
            P(both, None),
            P(both, None, None),
            P(both, None, None),
        ),
        out_specs=(P(both, None), P(None, both), P(both)),
        check_vma=False,
    )
```

```python
import functools

import jax
import jax.numpy as jnp
from jax import lax
from jax.experimental import pallas as pl
from jax.experimental.pallas import tpu as pltpu
from jax.sharding import PartitionSpec as P

STATES = 96
UNITS = 512
NODES = 24
MAXP = 16
VARS = 112
LANES = 128
GROUP = 8
STEPS = STATES // GROUP
SENT_ROWS = 8
FIRST = 7
WRITES = 8
MESH = pl.DeviceIdType.MESH
BF16 = jnp.bfloat16
F32 = jnp.float32


def dot(a, b, dims):
    return lax.dot_general(a, b, (dims, ((), ())), preferred_element_type=F32)


def nn(a, b):
    return dot(a, b, ((1,), (0,)))


def nt(a, b):
    return dot(a, b, ((1,), (1,)))


def tn(a, b):
    return dot(a, b, ((0,), (0,)))


def iota(shape, axis):
    return lax.broadcasted_iota(jnp.int32, shape, axis)


def split2(x):
    high = x.astype(BF16)
    return high, (x - high.astype(F32)).astype(BF16)


def split3(x):
    high = x.astype(BF16)
    rest = x - high.astype(F32)
    mid = rest.astype(BF16)
    return high, mid, (rest - mid.astype(F32)).astype(BF16)


def front(
    n_grp, n_blk,
    vars_any, w_in_t_any, w_out_any, linear_any, step_any, count_any, node_any, con_any,
    tangent_ref, path_ref, start_ref,
    vars_ref, w_in_t_ref, w_out_ref, linear_ref, step_ref, count_ref, node_ref, con_ref, in_sem,
    defect_ref, slopes, w_cols, l_cols, half_row, entry, msg1, recv1, msg2, recv2, send_rows, recv_rows,
    s1_send, s1_recv, s2_send, s2_recv, s3_send, s3_recv,
):
    grp, blk = lax.axis_index("grp"), lax.axis_index("blk")
    pairs = count_ref.shape[0] * count_ref.shape[1]
    traj = count_ref.shape[1]
    rows = vars_ref.shape[1]
    slots = pairs * MAXP

    sources = (vars_any, w_in_t_any, w_out_any, linear_any, step_any, count_any, node_any, con_any)
    targets = (vars_ref, w_in_t_ref, w_out_ref, linear_ref, step_ref, count_ref, node_ref, con_ref)
    loads = [pltpu.make_async_copy(a, b, in_sem.at[i]) for i, (a, b) in enumerate(zip(sources, targets))]
    for load in loads:
        load.start()

    barrier = pltpu.get_barrier_semaphore()

    @pl.loop(1, n_blk)
    def _(i):
        pl.semaphore_signal(barrier, inc=1, device_id={"blk": lax.rem(blk + i, n_blk)}, device_id_type=MESH)

    @pl.loop(1, n_grp)
    def _(i):
        pl.semaphore_signal(barrier, inc=1, device_id={"grp": lax.rem(grp + i, n_grp)}, device_id_type=MESH)

    for load in loads:
        load.wait()

    w_in_t = w_in_t_ref[...]
    w_out = w_out_ref[...]
    linear = linear_ref[...]
    preact = tn(w_in_t, vars_ref[...])
    th = jnp.tanh(preact)
    slopes[...] = 1.0 - th * th

    row_pair = iota((1, rows), 1) // NODES
    half = jnp.zeros((1, rows), F32)
    for e in range(pairs):
        half = jnp.where(row_pair == e, step_ref[e // traj, e % traj] * 0.5, half)
    half_row[...] = half

    scaled = slopes[...] * half
    high, low = split2(scaled)
    gram = nt(high, high) + 2.0 * nt(high, low)
    m_high, m_low = split2(tn(w_out, w_out) * gram)
    w_in = w_in_t.astype(F32).T
    w_in16 = w_in.astype(BF16)
    inner = nn(m_high, w_in16) + nn(m_low, w_in16)
    cross = jnp.sum(scaled * half, axis=1, keepdims=True) * tn(w_out, linear)
    linear32 = linear.astype(F32)
    column = jnp.sum(w_in * (inner + 2.0 * cross), axis=0, keepdims=True)
    column += jnp.sum(half * half) * jnp.sum(linear32 * linear32, axis=0, keepdims=True)

    own_total = jnp.int32(0)
    befores = []
    for e in range(pairs):
        befores.append(own_total)
        own_total += count_ref[e // traj, e % traj]
    tail = jnp.where(iota((1, LANES - VARS), 1) == 0, own_total.astype(F32), 0.0)
    message = jnp.concatenate([column, tail], axis=1)
    msg1[0] = message
    recv1[blk] = message

    pl.semaphore_wait(barrier, n_blk + n_grp - 2)

    def copy1(i):
        peer = lax.rem(blk + i, n_blk)
        return pltpu.make_async_remote_copy(
            src_ref=msg1.at[0], dst_ref=recv1.at[blk], send_sem=s1_send.at[peer], recv_sem=s1_recv.at[blk],
            device_id={"blk": peer}, device_id_type=MESH)

    @pl.loop(1, n_blk)
    def _(i):
        copy1(i).start()

    w_t = w_out.astype(F32).T
    l_t = linear32.T
    for g in range(STEPS):
        w_cols[g] = w_t[:, g * GROUP:(g + 1) * GROUP]
        l_cols[g] = l_t[:, g * GROUP:(g + 1) * GROUP]

    def main(g):
        for k in range(0, GROUP, 2):
            cols = w_cols[g]
            here = slopes[...]
            block = jnp.concatenate([here * cols[:, k:k + 1], here * cols[:, k + 1:k + 2]], axis=1)
            product = nn(w_in_t, block.astype(BF16))
            lin = l_cols[g]
            for j in range(2):
                part = product[:, j * rows:(j + 1) * rows] + lin[:, k + j:k + j + 1]
                defect_ref[g * GROUP + k + j] = part * half_row[...]

    slot_pair = iota((slots, 1), 0) // MAXP
    slot_k = iota((slots, 1), 0) % MAXP
    count = jnp.zeros((slots, 1), jnp.int32)
    before = jnp.zeros((slots, 1), jnp.int32)
    for e in range(pairs):
        count = jnp.where(slot_pair == e, count_ref[e // traj, e % traj], count)
        before = jnp.where(slot_pair == e, befores[e], before)
    number = jnp.where(slot_k < count, before + slot_k, -1)

    def by_slot(ref):
        table = ref[...].reshape(pairs, 1, MAXP).astype(F32)
        wide = jnp.broadcast_to(table, (pairs, MAXP, MAXP)).reshape(slots, MAXP)
        mine = iota((slots, MAXP), 1) == slot_k
        return jnp.sum(jnp.where(mine, wide, 0.0), axis=1, keepdims=True).astype(jnp.int32)

    node = slot_pair * NODES + by_slot(node_ref)
    con = by_slot(con_ref)
    pick_node = (iota((slots, rows), 1) == node).astype(F32).astype(BF16)
    pick_con = (iota((slots, STATES), 1) == con).astype(F32).astype(BF16)
    s_high, s_mid, s_low = split3(slopes[...])
    slope_rows = nt(pick_node, s_high) + (nt(pick_node, s_mid) + nt(pick_node, s_low))
    scaled_rows = (nn(pick_con, w_out) * slope_rows).astype(BF16)
    entry_rows = nt(scaled_rows, w_in_t) + nn(pick_con, linear)
    entry[...] = jnp.concatenate([entry_rows, jnp.zeros((slots, LANES - VARS), F32)], axis=1).astype(BF16)

    @pl.loop(0, FIRST)
    def _(g):
        main(g)

    @pl.loop(1, n_blk)
    def _(i):
        peer = lax.rem(blk + i, n_blk)
        pltpu.make_async_remote_copy(
            src_ref=msg1.at[0], dst_ref=recv1.at[peer], send_sem=s1_send.at[peer], recv_sem=s1_recv.at[peer],
            device_id={"blk": peer}, device_id_type=MESH).wait_recv()

    table = recv1[...].reshape(n_blk, LANES)
    message2 = jnp.sum(table, axis=0, keepdims=True)
    msg2[0] = message2
    recv2[grp] = message2

    def copy2(i):
        peer = lax.rem(grp + i, n_grp)
        return pltpu.make_async_remote_copy(
            src_ref=msg2.at[0], dst_ref=recv2.at[grp], send_sem=s2_send.at[peer], recv_sem=s2_recv.at[grp],
            device_id={"grp": peer}, device_id_type=MESH)

    @pl.loop(1, n_grp)
    def _(i):
        copy2(i).start()

    earlier = (iota((n_blk, n_blk), 1) < iota((n_blk, n_blk), 0)).astype(F32).astype(BF16)
    total32 = table[:, VARS:VARS + 1]
    firsts = nn(earlier, table.astype(BF16))[:, VARS:VARS + 1].astype(jnp.int32)
    totals = total32.astype(jnp.int32)
    mine = iota((n_blk, 1), 0) == blk
    first = jnp.sum(jnp.where(mine, firsts, 0))

    q = iota((1, n_blk * SENT_ROWS), 1)
    wanted = lax.rem(q // SENT_ROWS + n_blk * MAXP * pairs - first, n_blk) + n_blk * (q % SENT_ROWS)
    move = (number == wanted).astype(F32).astype(BF16)
    moved = tn(move, entry[...]).astype(BF16).reshape(n_blk, SENT_ROWS, LANES)
    send_rows[...] = moved

    def copy3(i):
        peer = lax.rem(blk + i, n_blk)
        return pltpu.make_async_remote_copy(
            src_ref=send_rows.at[peer], dst_ref=recv_rows.at[blk], send_sem=s3_send.at[peer], recv_sem=s3_recv.at[blk],
            device_id={"blk": peer}, device_id_type=MESH)

    @pl.loop(1, n_blk)
    def _(i):
        copy3(i).start()

    recv_rows[blk] = send_rows[blk]

    skip = lax.rem(blk + n_blk * MAXP * pairs - firsts, n_blk)
    slot0 = (firsts + skip) // n_blk
    live_rows = (totals - skip + n_blk - 1) // n_blk

    def by_row(x):
        return jnp.broadcast_to(x.astype(F32).reshape(n_blk, 1, 1), (n_blk, SENT_ROWS, 1)).reshape(n_blk * SENT_ROWS, 1).astype(jnp.int32)

    k_row = iota((n_blk * SENT_ROWS, 1), 0) % SENT_ROWS
    slot_row = jnp.where(k_row < by_row(live_rows), by_row(slot0) + k_row, -1)
    place = (iota((n_blk * SENT_ROWS, slots), 1) == slot_row).astype(F32).astype(BF16)

    @pl.loop(FIRST, STEPS)
    def _(g):
        main(g)

    @pl.loop(1, n_grp)
    def _(i):
        peer = lax.rem(grp + i, n_grp)
        pltpu.make_async_remote_copy(
            src_ref=msg2.at[0], dst_ref=recv2.at[peer], send_sem=s2_send.at[peer], recv_sem=s2_recv.at[peer],
            device_id={"grp": peer}, device_id_type=MESH).wait_recv()

    table2 = recv2[...].reshape(n_grp, LANES)
    earlier_groups = jnp.where(iota((n_grp, 1), 0) < grp, table2[:, VARS:VARS + 1], 0.0)
    start_ref[...] = jnp.full(start_ref.shape, jnp.sum(earlier_groups).astype(jnp.int32) + first)
    column_sq = jnp.sum(table2, axis=0, keepdims=True)
    entries = rows * n_grp * n_blk * STATES
    inverse = 1.0 / jnp.sqrt(column_sq / entries + 1e-06)
    inv = jnp.broadcast_to(inverse, (LANES, LANES)).T[:VARS]
    inv = jnp.concatenate([inv] * (rows // LANES), axis=1)

    for g in range(STEPS):
        block = (defect_ref[pl.ds(g * GROUP, GROUP)] * inv[None]).astype(BF16)
        tangent_ref[:, g * GROUP * VARS:(g + 1) * GROUP * VARS] = block.reshape(GROUP * VARS, rows).T

    @pl.loop(1, n_blk)
    def _(i):
        peer = lax.rem(blk + i, n_blk)
        pltpu.make_async_remote_copy(
            src_ref=send_rows.at[peer], dst_ref=recv_rows.at[peer], send_sem=s3_send.at[peer], recv_sem=s3_recv.at[peer],
            device_id={"blk": peer}, device_id_type=MESH).wait_recv()

    received = recv_rows[...].reshape(n_blk * SENT_ROWS, LANES)
    path_ref[...] = tn(received, place)[:VARS].astype(BF16)

    @pl.loop(1, n_blk)
    def _(i):
        copy1(i).wait_send()
        copy3(i).wait_send()

    @pl.loop(1, n_grp)
    def _(i):
        copy2(i).wait_send()


def back(tangent_ref, path_ref, start_ref, tangent_any, path_any, start_any, first, sem):
    first[...] = jnp.full((1,), jnp.max(start_ref[...]))
    rows = tangent_ref.shape[0] // WRITES
    copies = [pltpu.make_async_copy(first, start_any, sem.at[WRITES + 1]), pltpu.make_async_copy(path_ref, path_any, sem.at[WRITES])]
    for i in range(WRITES):
        part = pl.ds(i * rows, rows)
        copies.append(pltpu.make_async_copy(tangent_ref.at[part], tangent_any.at[part], sem.at[i]))
    for copy in copies:
        copy.start()
    for copy in copies:
        copy.wait()


def local(n_grp, n_blk, node_vars, w_in, w_out, linear_part, step_len, path_count, path_node, path_con):
    rows = node_vars.shape[1]
    slots = path_count.shape[0] * path_count.shape[1] * MAXP
    vmem = pl.BlockSpec(memory_space=pltpu.VMEM)
    dma = pltpu.SemaphoreType.DMA
    hbm = pl.BlockSpec(memory_space=pl.ANY)
    operands = (node_vars, w_in.T, w_out, linear_part, step_len, path_count, path_node, path_con)
    scalars = (4, 5)
    homes = [(pltpu.SMEM if i in scalars else pltpu.VMEM)(x.shape, x.dtype) for i, x in enumerate(operands)]
    done = pl.pallas_call(
        functools.partial(front, n_grp, n_blk),
        out_shape=(
            pltpu.VMEM((rows, STATES * VARS), BF16),
            pltpu.VMEM((VARS, slots), BF16),
            pltpu.VMEM((8, LANES), jnp.int32),
        ),
        in_specs=[hbm] * len(operands),
        out_specs=(vmem, vmem, vmem),
        scratch_shapes=homes + [
            dma((len(operands),)),
            pltpu.VMEM((STATES, VARS, rows), F32),
            pltpu.VMEM((UNITS, rows), F32),
            pltpu.VMEM((STEPS, UNITS, GROUP), F32),
            pltpu.VMEM((STEPS, VARS, GROUP), F32),
            pltpu.VMEM((1, rows), F32),
            pltpu.VMEM((slots, LANES), BF16),
            pltpu.VMEM((1, 1, LANES), F32),
            pltpu.VMEM((n_blk, 1, LANES), F32),
            pltpu.VMEM((1, 1, LANES), F32),
            pltpu.VMEM((n_grp, 1, LANES), F32),
            pltpu.VMEM((n_blk, SENT_ROWS, LANES), BF16),
            pltpu.VMEM((n_blk, SENT_ROWS, LANES), BF16),
            dma((n_blk,)), dma((n_blk,)), dma((n_grp,)), dma((n_grp,)), dma((n_blk,)), dma((n_blk,)),
        ],
        compiler_params=pltpu.CompilerParams(collective_id=0, has_side_effects=True, vmem_limit_bytes=50 * 2**20),
        name="front",
    )(*operands)
    return pl.pallas_call(
        back,
        out_shape=(
            jax.ShapeDtypeStruct((rows, STATES * VARS), BF16),
            jax.ShapeDtypeStruct((VARS, slots), BF16),
            jax.ShapeDtypeStruct((1,), jnp.int32),
        ),
        in_specs=[vmem] * 3,
        out_specs=(hbm, hbm, hbm),
        scratch_shapes=[pltpu.VMEM((1,), jnp.int32), dma((WRITES + 2,))],
        compiler_params=pltpu.CompilerParams(vmem_limit_bytes=2**20),
        name="back",
    )(*done)


def solution(mesh):
    both = ("grp", "blk")
    return jax.shard_map(
        functools.partial(local, mesh.shape["grp"], mesh.shape["blk"]),
        mesh=mesh,
        in_specs=(
            P(None, both),
            P(),
            P(),
            P(),
            P(both, None),
            P(both, None),
            P(both, None, None),
            P(both, None, None),
        ),
        out_specs=(P(both, None), P(None, both), P(both)),
        check_vma=False,
    )
```

```python
import functools

import jax
import jax.numpy as jnp
from jax import lax
from jax.experimental import pallas as pl
from jax.experimental.pallas import tpu as pltpu
from jax.sharding import PartitionSpec as P

STATES = 96
UNITS = 512
NODES = 24
MAXP = 16
VARS = 112
LANES = 128
GROUP = 16
STEPS = STATES // GROUP
PAIR = 2
SENT_ROWS = 8
EARLY = 3
WRITES = 24
MESH = pl.DeviceIdType.MESH
BF16 = jnp.bfloat16
F32 = jnp.float32


def dot(a, b, dims):
    return lax.dot_general(a, b, (dims, ((), ())), preferred_element_type=F32)


def nn(a, b):
    return dot(a, b, ((1,), (0,)))


def nt(a, b):
    return dot(a, b, ((1,), (1,)))


def tn(a, b):
    return dot(a, b, ((0,), (0,)))


def iota(shape, axis):
    return lax.broadcasted_iota(jnp.int32, shape, axis)


def split2(x):
    high = x.astype(BF16)
    return high, (x - high.astype(F32)).astype(BF16)


def split3(x):
    high = x.astype(BF16)
    rest = x - high.astype(F32)
    mid = rest.astype(BF16)
    return high, mid, (rest - mid.astype(F32)).astype(BF16)


def front(
    n_grp, n_blk,
    vars_any, w_in_t_any, w_out_any, linear_any, step_any, count_any, node_any, con_any,
    defect_ref, inv_ref, half_ref, path_ref, start_ref,
    vars_ref, w_in_t_ref, w_out_ref, linear_ref, step_ref, count_ref, node_ref, con_ref, in_sem,
    held, squares, slopes, w_rows, l_rows, half_row, entry, send_rows, recv_rows,
    count_out, count_in, total_out, total_in, sum_out, sum_in, all_out, all_in,
    row_sems, count_sems, total_sems, sum_sems, all_sems,
):
    grp, blk = lax.axis_index("grp"), lax.axis_index("blk")
    pairs = count_ref.shape[0] * count_ref.shape[1]
    traj = count_ref.shape[1]
    rows = vars_ref.shape[1]
    slots = pairs * MAXP

    sources = (vars_any, w_in_t_any, w_out_any, linear_any, step_any, count_any, node_any, con_any)
    targets = (vars_ref, w_in_t_ref, w_out_ref, linear_ref, step_ref, count_ref, node_ref, con_ref)
    loads = [pltpu.make_async_copy(a, b, in_sem.at[i]) for i, (a, b) in enumerate(zip(sources, targets))]
    for load in loads:
        load.start()

    barrier = pltpu.get_barrier_semaphore()

    @pl.loop(1, n_blk)
    def _(i):
        pl.semaphore_signal(barrier, inc=1, device_id={"blk": lax.rem(blk + i, n_blk)}, device_id_type=MESH)

    @pl.loop(1, n_grp)
    def _(i):
        pl.semaphore_signal(barrier, inc=1, device_id={"grp": lax.rem(grp + i, n_grp)}, device_id_type=MESH)

    for load in loads:
        load.wait()

    w_in_t = w_in_t_ref[...]
    w_out = w_out_ref[...]
    linear = linear_ref[...]
    preact = tn(w_in_t, vars_ref[...])
    th = jnp.tanh(preact)
    slopes[...] = 1.0 - th * th

    row_pair = iota((1, rows), 1) // NODES
    half = jnp.zeros((1, rows), F32)
    for e in range(pairs):
        half = jnp.where(row_pair == e, step_ref[e // traj, e % traj] * 0.5, half)
    half_row[...] = half

    own_total = jnp.int32(0)
    befores = []
    for e in range(pairs):
        befores.append(own_total)
        own_total += count_ref[e // traj, e % traj]
    own = jnp.full((1, LANES), own_total.astype(F32))
    count_out[0] = own
    count_in[blk] = own

    w_rows[...] = w_out.astype(F32).reshape(STEPS, GROUP, UNITS)
    l_rows[...] = linear.astype(F32).reshape(STEPS, GROUP, VARS)
    squares[...] = jnp.zeros_like(squares)

    def column_of(ref, g, k):
        row = ref[g, k:k + 1, :].astype(BF16)
        return jnp.broadcast_to(row, (LANES, row.shape[1])).T.astype(F32)

    def main(g):
        for k in range(0, GROUP, PAIR):
            tiles = []
            for j in range(PAIR):
                w = column_of(w_rows, g, k + j)
                for q in range(0, rows, LANES):
                    tiles.append((slopes[:, q:q + LANES] * w).astype(BF16))
            product = nn(w_in_t, jnp.concatenate(tiles, axis=1))
            lins = [column_of(l_rows, g, k + j) for j in range(PAIR)]
            for q in range(0, rows, LANES):
                square = squares[:, q:q + LANES]
                for j in range(PAIR):
                    part = product[:, j * rows + q:j * rows + q + LANES] + lins[j]
                    square += part * part
                    held[g * GROUP + k + j, :, q:q + LANES] = part
                squares[:, q:q + LANES] = square

    ahead = jnp.maximum(STEPS - lax.rem(blk, 8), EARLY)

    @pl.loop(0, ahead)
    def _(g):
        main(g)

    def exchange(axis, n, me, source, target, sems, by_peer):
        def copy(i, there):
            peer = lax.rem(me + i, n)
            place = peer if there else me
            return pltpu.make_async_remote_copy(
                src_ref=source.at[peer if by_peer else 0], dst_ref=target.at[place],
                send_sem=sems.at[0, peer], recv_sem=sems.at[1, place],
                device_id={axis: peer}, device_id_type=MESH)

        def start():
            for i in range(1, n):
                copy(i, False).start()

        def receive():
            for i in range(1, n):
                copy(i, True).wait_recv()

        def finish():
            @pl.loop(1, n)
            def _(i):
                copy(i, False).wait_send()

        return start, receive, finish

    counts = exchange("blk", n_blk, blk, count_out, count_in, count_sems, False)
    totals_x = exchange("grp", n_grp, grp, total_out, total_in, total_sems, False)
    sums = exchange("grp", n_grp, grp, sum_out, sum_in, sum_sems, False)
    alls = exchange("blk", n_blk, blk, all_out, all_in, all_sems, False)
    path = exchange("blk", n_blk, blk, send_rows, recv_rows, row_sems, True)

    pl.semaphore_wait(barrier, n_blk + n_grp - 2)
    counts[0]()

    @pl.loop(ahead, STEPS)
    def _(g):
        main(g)

    half = half_row[...]
    weighted = squares[...] * (half * half)
    weighted = sum(weighted[:, q:q + LANES] for q in range(0, rows, LANES))
    column = jnp.sum(weighted.T, axis=0, keepdims=True)
    own_sum = jnp.concatenate([column, jnp.zeros((1, LANES - VARS), F32)], axis=1)
    sum_out[0] = own_sum
    sum_in[grp] = own_sum
    sums[0]()

    slot_pair = iota((slots, 1), 0) // MAXP
    slot_k = iota((slots, 1), 0) % MAXP
    count = jnp.zeros((slots, 1), jnp.int32)
    before = jnp.zeros((slots, 1), jnp.int32)
    for e in range(pairs):
        count = jnp.where(slot_pair == e, count_ref[e // traj, e % traj], count)
        before = jnp.where(slot_pair == e, befores[e], before)
    number = jnp.where(slot_k < count, before + slot_k, -1)

    def by_slot(ref):
        table = ref[...].reshape(pairs, 1, MAXP).astype(F32)
        wide = jnp.broadcast_to(table, (pairs, MAXP, MAXP)).reshape(slots, MAXP)
        mine = iota((slots, MAXP), 1) == slot_k
        return jnp.sum(jnp.where(mine, wide, 0.0), axis=1, keepdims=True).astype(jnp.int32)

    node = slot_pair * NODES + by_slot(node_ref)
    con = by_slot(con_ref)
    pick_node = (iota((slots, rows), 1) == node).astype(F32).astype(BF16)
    pick_con = (iota((slots, STATES), 1) == con).astype(F32).astype(BF16)
    s_high, s_mid, s_low = split3(slopes[...])
    slope_rows = nt(pick_node, s_high) + (nt(pick_node, s_mid) + nt(pick_node, s_low))
    scaled_rows = (nn(pick_con, w_out) * slope_rows).astype(BF16)
    entry_rows = nt(scaled_rows, w_in_t) + nn(pick_con, linear)
    entry[...] = jnp.concatenate([entry_rows, jnp.zeros((slots, LANES - VARS), F32)], axis=1).astype(BF16)

    counts[1]()
    table = count_in[...].reshape(n_blk, LANES)
    group_total = jnp.sum(table, axis=0, keepdims=True)
    total_out[0] = group_total
    total_in[grp] = group_total
    totals_x[0]()

    earlier = (iota((n_blk, n_blk), 1) < iota((n_blk, n_blk), 0)).astype(F32).astype(BF16)
    firsts = nn(earlier, table.astype(BF16))[:, :1].astype(jnp.int32)
    totals = table[:, :1].astype(jnp.int32)
    mine = iota((n_blk, 1), 0) == blk
    first = jnp.sum(jnp.where(mine, firsts, 0))

    q = iota((1, n_blk * SENT_ROWS), 1)
    wanted = lax.rem(q // SENT_ROWS + n_blk * MAXP * pairs - first, n_blk) + n_blk * (q % SENT_ROWS)
    move = (number == wanted).astype(F32).astype(BF16)
    send_rows[...] = tn(move, entry[...]).astype(BF16).reshape(n_blk, SENT_ROWS, LANES)
    path[0]()
    recv_rows[blk] = send_rows[blk]

    sums[1]()
    group_sum = jnp.sum(sum_in[...].reshape(n_grp, LANES), axis=0, keepdims=True)
    all_out[0] = group_sum
    all_in[blk] = group_sum
    alls[0]()

    @pl.loop(0, STEPS)
    def _(g):
        block = held[pl.ds(g * GROUP, GROUP)].reshape(GROUP * VARS, rows)
        defect_ref[:, pl.ds(pl.multiple_of(g * GROUP * VARS, LANES), GROUP * VARS)] = block.T

    half_ref[...] = jnp.broadcast_to(half_row[...], (LANES, rows)).T

    skip = lax.rem(blk + n_blk * MAXP * pairs - firsts, n_blk)
    slot0 = (firsts + skip) // n_blk
    live_rows = (totals - skip + n_blk - 1) // n_blk

    def by_row(x):
        return jnp.broadcast_to(x.astype(F32).reshape(n_blk, 1, 1), (n_blk, SENT_ROWS, 1)).reshape(n_blk * SENT_ROWS, 1).astype(jnp.int32)

    k_row = iota((n_blk * SENT_ROWS, 1), 0) % SENT_ROWS
    slot_row = jnp.where(k_row < by_row(live_rows), by_row(slot0) + k_row, -1)
    place = (iota((n_blk * SENT_ROWS, slots), 1) == slot_row).astype(F32).astype(BF16)

    totals_x[1]()
    earlier_groups = jnp.where(iota((n_grp, 1), 0) < grp, total_in[...].reshape(n_grp, LANES)[:, :1], 0.0)
    start_ref[...] = jnp.full(start_ref.shape, jnp.sum(earlier_groups).astype(jnp.int32) + first)

    path[1]()
    received = recv_rows[...].reshape(n_blk * SENT_ROWS, LANES)
    path_ref[...] = tn(received, place)[:VARS].astype(BF16)
    for each in (counts, totals_x, sums, path):
        each[2]()

    alls[1]()
    column_sq = jnp.sum(all_in[...].reshape(n_blk, LANES), axis=0, keepdims=True)
    entries = rows * n_grp * n_blk * STATES
    inverse = 1.0 / jnp.sqrt(column_sq[:, :VARS] / entries + 1e-06)
    inv_ref[...] = jnp.concatenate([inverse] * GROUP, axis=1)
    alls[2]()


def back(defect_ref, inv_ref, half_ref, path_ref, start_ref, tangent_any, path_any, start_any, first, tangent, sem):
    first[...] = jnp.full((1,), jnp.max(start_ref[...]))
    small = [pltpu.make_async_copy(first, start_any, sem.at[WRITES + 1]), pltpu.make_async_copy(path_ref, path_any, sem.at[WRITES])]
    for copy in small:
        copy.start()
    rows = tangent.shape[0] // WRITES
    inv = inv_ref[...]

    def write(i):
        part = pl.ds(pl.multiple_of(i * rows, rows), rows)
        return pltpu.make_async_copy(tangent.at[part], tangent_any.at[part], sem.at[i])

    @pl.loop(0, WRITES)
    def _(i):
        part = pl.ds(pl.multiple_of(i * rows, rows), rows)
        scale = jnp.concatenate([half_ref[part]] * (GROUP * VARS // LANES), axis=1) * inv
        for c in range(0, STATES * VARS, GROUP * VARS):
            tangent[part, c:c + GROUP * VARS] = (defect_ref[part, c:c + GROUP * VARS] * scale).astype(BF16)
        write(i).start()

    for copy in small:
        copy.wait()

    @pl.loop(0, WRITES)
    def _(i):
        write(i).wait()


def local(n_grp, n_blk, node_vars, w_in, w_out, linear_part, step_len, path_count, path_node, path_con):
    rows = node_vars.shape[1]
    slots = path_count.shape[0] * path_count.shape[1] * MAXP
    vmem = pl.BlockSpec(memory_space=pltpu.VMEM)
    dma = pltpu.SemaphoreType.DMA
    hbm = pl.BlockSpec(memory_space=pl.ANY)
    operands = (node_vars, w_in.T, w_out, linear_part, step_len, path_count, path_node, path_con)
    scalars = (4, 5)
    homes = [(pltpu.SMEM if i in scalars else pltpu.VMEM)(x.shape, x.dtype) for i, x in enumerate(operands)]
    pair = lambda n: dma((2, n))
    line = lambda n: pltpu.VMEM((n, 1, LANES), F32)
    done = pl.pallas_call(
        functools.partial(front, n_grp, n_blk),
        out_shape=(
            pltpu.VMEM((rows, STATES * VARS), F32),
            pltpu.VMEM((1, GROUP * VARS), F32),
            pltpu.VMEM((rows, LANES), F32),
            pltpu.VMEM((VARS, slots), BF16),
            pltpu.VMEM((8, LANES), jnp.int32),
        ),
        in_specs=[hbm] * len(operands),
        out_specs=(vmem,) * 5,
        scratch_shapes=homes + [
            dma((len(operands),)),
            pltpu.VMEM((STATES, VARS, rows), F32),
            pltpu.VMEM((VARS, rows), F32),
            pltpu.VMEM((UNITS, rows), F32),
            pltpu.VMEM((STEPS, GROUP, UNITS), F32),
            pltpu.VMEM((STEPS, GROUP, VARS), F32),
            pltpu.VMEM((1, rows), F32),
            pltpu.VMEM((slots, LANES), BF16),
            pltpu.VMEM((n_blk, SENT_ROWS, LANES), BF16),
            pltpu.VMEM((n_blk, SENT_ROWS, LANES), BF16),
            line(1), line(n_blk), line(1), line(n_grp), line(1), line(n_grp), line(1), line(n_blk),
            pair(n_blk), pair(n_blk), pair(n_grp), pair(n_grp), pair(n_blk),
        ],
        compiler_params=pltpu.CompilerParams(
            collective_id=0, has_side_effects=True, vmem_limit_bytes=42 * 2**20),
        name="front",
    )(*operands)
    return pl.pallas_call(
        back,
        out_shape=(
            jax.ShapeDtypeStruct((rows, STATES * VARS), BF16),
            jax.ShapeDtypeStruct((VARS, slots), BF16),
            jax.ShapeDtypeStruct((1,), jnp.int32),
        ),
        in_specs=[vmem] * 5,
        out_specs=(hbm, hbm, hbm),
        scratch_shapes=[pltpu.VMEM((1,), jnp.int32), pltpu.VMEM((rows, STATES * VARS), BF16), dma((WRITES + 2,))],
        compiler_params=pltpu.CompilerParams(vmem_limit_bytes=16 * 2**20),
        name="back",
    )(*done)


def solution(mesh):
    both = ("grp", "blk")
    return jax.shard_map(
        functools.partial(local, mesh.shape["grp"], mesh.shape["blk"]),
        mesh=mesh,
        in_specs=(
            P(None, both),
            P(),
            P(),
            P(),
            P(both, None),
            P(both, None),
            P(both, None, None),
            P(both, None, None),
        ),
        out_specs=(P(both, None), P(None, both), P(both)),
        check_vma=False,
    )
```
